32 devices in a mesh: win: 4 (over z), slab: 8 (over y, x, core).
Axes of the slice: x: 2, y: 2, z: 4, core: 2. Of those that a mesh axis runs over, the one named last changes fastest.
Arguments:
- lambdas: float32 [16], P('win'), parts along dimension 0, may hold values from 0 to 1
- charge_a: float32 [16, 4096], P('win', 'slab'), parts along dimension 0, may hold values from -3 to 3
- charge_b: float32 [16, 4096], P('win', 'slab'), parts along dimension 0, may hold values from -3 to 3
- perturbed: int32 [16, 4096], P('win', 'slab'), parts along dimension 0, may hold values 0 or 1
- grid_index: int32 [3, 16, 4096], P(None, 'win', 'slab'), parts along dimension 1, may hold values from 0 to 127, as said below
- spline_weights: float32 [3, 4, 16, 4096], P(None, None, 'win', 'slab'), parts along dimension 2, may hold values from 0 to 1, as said below
- spline_slopes: float32 [3, 4, 16, 4096], P(None, None, 'win', 'slab'), parts along dimension 2, may hold values from -1 to 1, as said below
Outputs:
- forces: float32 [3, 16, 4096], P(None, 'win', 'slab'), parts along dimension 1
- energy: float32 [16], P('win'), parts along dimension 0
- lambda_slope: float32 [16], P('win'), parts along dimension 0
The draws below stay inside these ranges and needn't reach their ends.
There are 4 independent parts, one for each index of `win`. The reference program is written for one: setup_inputs(seed, part) draws one part's arguments, and reference() takes and returns one part's arrays. A program takes and returns all parts, laid end to end along the dimension named above; each array names one. Nothing has to cross between parts.
Inputs may be any that keep to these rules, and one draw needn't show every extreme that they name: `grid_index`: the z index of atom i lies in the planes of the slab index that holds it: from (i // 512) * 16 to that plus 16 - 1. `spline_weights`: along each dimension the four weights are the cubic B-spline values (1-u)^3/6, (3u^3-6u^2+4)/6, (-3u^3+3u^2+3u+1)/6, u^3/6 of the atom's fractional offset u in [0, 1). `spline_slopes`: the derivatives in u of spline_weights at the same offsets.
All inputs are finite; a program needn't handle non-finite values. No bound on the sum of `perturbed` on one device may be relied on, other than what follows from the above.
Results may differ from the reference program's by a relative error of at most 0.0003.
Values sent between devices are 32-bit elements; how exact they have to be, the bound alone decides.
A program may use at most 64 MiB of HBM per device.

```python
import math
import jax
import jax.numpy as jnp

NX = 128
NY = 128
NZ = 128
WINS = 4
ATOM_DEV = 512
ATOMS = 4096
SLAB_Z = 16


def spline_parts(key):
    fraction = jax.random.uniform(jax.random.fold_in(key, 17), (3, WINS, ATOMS), jnp.float32)
    remain = 1.0 - fraction
    weights = jnp.stack([remain ** 3 / 6.0, (3.0 * fraction ** 3 - 6.0 * fraction ** 2 + 4.0) / 6.0, (-3.0 * fraction ** 3 + 3.0 * fraction ** 2 + 3.0 * fraction + 1.0) / 6.0, fraction ** 3 / 6.0], axis=1)
    slopes = jnp.stack([-remain ** 2 / 2.0, (3.0 * fraction ** 2 - 4.0 * fraction) / 2.0, (-3.0 * fraction ** 2 + 2.0 * fraction + 1.0) / 2.0, fraction ** 2 / 2.0], axis=1)
    return (weights, slopes)


def draw_spline_weights(key, part):
    return spline_parts(key)[0].astype(jnp.float32)


def draw_spline_slopes(key, part):
    return spline_parts(key)[1].astype(jnp.float32)


def draw_grid_index(key, part):
    subkeys = jax.random.split(jax.random.fold_in(key, 5), 3)
    column = jax.random.randint(subkeys[0], (WINS, ATOMS), 0, NX)
    row_cell = jax.random.randint(subkeys[1], (WINS, ATOMS), 0, NY)
    owners = jnp.arange(ATOMS, dtype=jnp.int32) // ATOM_DEV
    depths = owners[None, :] * SLAB_Z + jax.random.randint(subkeys[2], (WINS, ATOMS), 0, SLAB_Z)
    return jnp.stack([column, row_cell, depths]).astype(jnp.int32)


def touch_ends(drawn, own_key, smallest, largest):
    longest = drawn.shape.index(max(drawn.shape))
    spots = []
    for shift in (0, 1):
        where = [jax.random.randint(jax.random.fold_in(own_key, axis), (), 0, length) for axis, length in enumerate(drawn.shape)]
        where[longest] = (where[longest] + shift) % drawn.shape[longest]
        spots.append(tuple(where))
    return drawn.at[spots[0]].set(smallest).at[spots[1]].set(largest)


def steps_of(own_key, dims, pieces, smallest, top_value):
    loudness, own = 1.0, jax.random.fold_in(own_key, 6)
    for position, parts in pieces:
        heights = jnp.exp(jax.random.uniform(jax.random.fold_in(own, position), (parts,), jnp.float32, smallest / len(pieces), top_value / len(pieces)))
        loudness = loudness * jnp.repeat(heights, dims[position] // parts).reshape([-1 if axis == position else 1 for axis in range(len(dims))])
    return loudness


def bell_draw(rng, extent, spread, reach, shards=(), held_as=jnp.bfloat16):
    entries = spread * jax.random.normal(rng, extent, jnp.float32)
    if shards:
        entries = entries * steps_of(rng, extent, shards, -0.22, 0.18)
    return jnp.clip(entries, -reach, reach).astype(held_as)


def setup_inputs(seed: int = 0, part: int = 0) -> dict:
    seeds = jax.random.split(jax.random.key(seed), 8)
    part_splits = jax.random.split(jax.random.fold_in(seeds[7], part), 8)
    return {
        "lambdas": jnp.clip(jax.random.uniform(part_splits[0], (WINS,), jnp.float32, 0.0, 1.0), 0.0, 1.0),
        "charge_a": bell_draw(part_splits[1], (WINS, ATOMS), 0.5, 3.0, ((1, 8),), jnp.float32),
        "charge_b": bell_draw(part_splits[2], (WINS, ATOMS), 0.5, 3.0, ((1, 8),), jnp.float32),
        "perturbed": touch_ends((jax.random.randint(part_splits[3], (WINS, ATOMS), 0, 4) < 1).astype(jnp.int32), jax.random.fold_in(part_splits[3], 1), 0, 1),
        "grid_index": draw_grid_index(jax.random.fold_in(jax.random.fold_in(seeds[7], part), 71), part),
        "spline_weights": draw_spline_weights(jax.random.fold_in(jax.random.fold_in(seeds[7], part), 71), part),
        "spline_slopes": draw_spline_slopes(jax.random.fold_in(jax.random.fold_in(seeds[7], part), 71), part),
    }


gauss_width = 2.0


def frequency(length):
    counter = jnp.arange(length, dtype=jnp.int32)
    return jnp.where(counter >= length // 2, counter - length, counter).astype(jnp.float32) / length


def influence_table():
    along_z = frequency(NZ)[:, None, None]
    along_x = frequency(NX)[None, :, None]
    along_y = frequency(NY)[None, None, :]
    squared = along_z * along_z + along_x * along_x + along_y * along_y
    positive = squared > 0
    safe_value = jnp.where(positive, squared, jnp.float32(1.0))
    return jnp.where(positive, jnp.exp(-gauss_width * squared) / (math.pi * NX * NY * NZ * safe_value), jnp.float32(0.0))


def reference(lambdas, charge_a, charge_b, perturbed, grid_index, spline_weights, spline_slopes):
    influence = influence_table()
    offsets = jnp.arange(4, dtype=jnp.int32)
    force_list = []
    energy_list = []
    slope_list = []
    for window in range(WINS):
        flag_values = perturbed[window].astype(jnp.float32)
        charge = charge_a[window] + flag_values * lambdas[window] * (charge_b[window] - charge_a[window])
        charge_step = flag_values * (charge_b[window] - charge_a[window])
        cells_z = ((grid_index[2, window][:, None] + offsets[None, :]) % NZ)[:, :, None, None]
        cells_x = ((grid_index[0, window][:, None] + offsets[None, :]) % NX)[:, None, :, None]
        cells_y = ((grid_index[1, window][:, None] + offsets[None, :]) % NY)[:, None, None, :]
        weight_z = spline_weights[2, :, window].T[:, :, None, None]
        weight_x = spline_weights[0, :, window].T[:, None, :, None]
        weight_y = spline_weights[1, :, window].T[:, None, None, :]
        slope_z = spline_slopes[2, :, window].T[:, :, None, None]
        slope_x = spline_slopes[0, :, window].T[:, None, :, None]
        slope_y = spline_slopes[1, :, window].T[:, None, None, :]
        stencil = weight_z * weight_x * weight_y
        charge_grid = jnp.zeros((NZ, NX, NY), jnp.float32).at[cells_z, cells_x, cells_y].add(charge[:, None, None, None] * stencil)
        spectrum = jnp.fft.fftn(charge_grid)
        power_map = jnp.real(spectrum) ** 2 + jnp.imag(spectrum) ** 2
        energy_list.append(0.5 * jnp.sum(influence * power_map))
        potential = jnp.real(jnp.fft.ifftn(influence * spectrum)) * (NX * NY * NZ)
        sampled = potential[cells_z, cells_x, cells_y]
        atom_value = jnp.sum(stencil * sampled, axis=(1, 2, 3))
        force_x = -charge * jnp.sum(weight_z * slope_x * weight_y * sampled, axis=(1, 2, 3))
        force_y = -charge * jnp.sum(weight_z * weight_x * slope_y * sampled, axis=(1, 2, 3))
        force_z = -charge * jnp.sum(slope_z * weight_x * weight_y * sampled, axis=(1, 2, 3))
        force_list.append(jnp.stack([force_x, force_y, force_z]))
        slope_list.append(jnp.sum(charge_step * atom_value))
    forces = jnp.stack(force_list, axis=1)
    energy = jnp.stack(energy_list) / ATOMS
    lambda_slope = jnp.stack(slope_list) / ATOMS
    return (forces, energy, lambda_slope)
```

```python
import functools

import jax
import jax.numpy as jnp
import numpy as np
from jax import lax
from jax.experimental import pallas as pl
from jax.experimental.pallas import tpu as pltpu
from jax.sharding import PartitionSpec as P

NX = 128
NY = 128
NZ = 128
REACH = 3

gauss_width = 2.0

CHARGE, STEP, CELL_X, CELL_Y, CELL_Z = 0, 1, 2, 3, 4
WX, WY, WZ, SX, SY, SZ = 8, 12, 16, 20, 24, 28
ROWS = 32


def passed_along(value, axis, steps):
    count = lax.axis_size(axis)
    pairs = [(source, (source + steps) % count) for source in range(count)]
    return lax.ppermute(value, axis, pairs)


def trig(length):
    counter = np.arange(length)
    angles = (np.outer(counter, counter) % length) * (2.0 * np.pi / length)
    return np.cos(angles), np.sin(angles)


def halves(table):
    table = table.astype(np.float32)
    high = table.astype(jnp.bfloat16)
    low = (table - high.astype(np.float32)).astype(jnp.bfloat16)
    return jnp.asarray(np.stack([high, low]))


def split(value):
    high = value.astype(jnp.bfloat16)
    return high, (value - high.astype(jnp.float32)).astype(jnp.bfloat16)


def dot3(left, right, dims=((1,), (0,))):
    one = functools.partial(
        lax.dot_general, dimension_numbers=(dims, ((), ())), preferred_element_type=jnp.float32
    )
    return one(left[0], right[0]) + (one(left[0], right[1]) + one(left[1], right[0]))


def stencil_rows(record, cell_row, weight_row, length):
    first = record[cell_row : cell_row + 1].astype(jnp.int32)
    cells = lax.broadcasted_iota(jnp.int32, (length, record.shape[1]), 0)
    away = cells - first
    away = jnp.where(away < 0, away + length, away)
    result = jnp.zeros(away.shape, jnp.float32)
    for offset in range(4):
        row = weight_row + offset
        result = jnp.where(away == offset, record[row : row + 1], result)
    return result


def plane_row(record, weight_row, plane, shift):
    away = plane + shift - record[CELL_Z : CELL_Z + 1].astype(jnp.int32)
    result = jnp.zeros(away.shape, jnp.float32)
    for offset in range(4):
        row = weight_row + offset
        result = jnp.where(away == offset, record[row : row + 1], result)
    return result


def planes_reached(distance, depth):
    if distance == 0:
        return depth
    return min(depth, depth + REACH - distance * depth)


def spread_kernel(depth, columns, native, atoms_ref, ty_ref, tx_ref, out_ref, grid_ref):
    sets = atoms_ref.shape[0]
    for part in range(2):
        lanes = slice(part * NY, (part + 1) * NY)
        for distance in range(sets):
            record = atoms_ref[distance, part]
            rows_x = stencil_rows(record, CELL_X, WX, NX)
            rows_y = split(stencil_rows(record, CELL_Y, WY, NY))
            charge = record[CHARGE : CHARGE + 1]

            def one_plane(plane, carry):
                strength = plane_row(record, WZ, plane, distance * depth) * charge
                spread = dot3(split(rows_x * strength), rows_y, ((1,), (1,)))
                if distance == 0:
                    grid_ref[plane, :, lanes] = spread
                else:
                    grid_ref[plane, :, lanes] += spread
                return carry

            lax.fori_loop(0, planes_reached(distance, depth), one_plane, 0)

    table_y = (ty_ref[0], ty_ref[1])
    table_x = (tx_ref[0], tx_ref[1])

    def transform(plane, carry):
        along_y = dot3(split(grid_ref[plane]), table_y)
        real, imaginary = along_y[:, :NY], along_y[:, NY:]
        stacked = jnp.concatenate(
            [along_y, jnp.concatenate([imaginary, -real], axis=1)], axis=0
        )
        both = dot3(table_x, split(stacked))
        for part in range(2):
            lanes = slice(part * NY, (part + 1) * NY)
            if native:
                for owner in range(NX // columns):
                    out_ref[owner, part, pl.ds(plane, columns, stride=depth), :] = both[
                        owner * columns : (owner + 1) * columns, lanes
                    ]
            else:
                out_ref[plane, part] = both[:, lanes]
        return carry

    lax.fori_loop(0, depth, transform, 0)


def column_kernel(columns, in_ref, influence_ref, forward_ref, inverse_ref, out_ref):
    sources = in_ref.shape[0]
    depth = in_ref.shape[2] // columns
    group = 2 if columns % 2 == 0 else 1
    forward = (forward_ref[0], forward_ref[1])
    inverse = (inverse_ref[0], inverse_ref[1])

    def one_group(step, carry):
        sides = []
        for k in range(group):
            start = pl.multiple_of((step * group + k) * depth, depth)
            sides.append(
                jnp.concatenate(
                    [
                        in_ref[source, part, pl.ds(start, depth), :]
                        for part in range(2)
                        for source in range(sources)
                    ],
                    axis=0,
                )
            )
        spectrum = dot3(forward, split(jnp.concatenate(sides, axis=1)))
        factor = jnp.concatenate([influence_ref[step * group + k] for k in range(group)], axis=1)
        scaled = spectrum * jnp.concatenate([factor, factor], axis=0)
        back = dot3(inverse, split(scaled))
        for k in range(group):
            start = pl.multiple_of((step * group + k) * depth, depth)
            for part in range(2):
                for source in range(sources):
                    top = part * NZ + source * depth
                    out_ref[source, part, pl.ds(start, depth), :] = back[
                        top : top + depth, k * NY : (k + 1) * NY
                    ]
        return carry

    lax.fori_loop(0, columns // group, one_group, 0)


def sample_kernel(
    depth, columns, native, in_ref, atoms_ref, ty_ref, tx_ref, out_ref, high_ref, low_ref, sums_ref
):
    sets = atoms_ref.shape[0]
    atoms = atoms_ref.shape[3]
    table_y = (ty_ref[0], ty_ref[1])
    table_x = (tx_ref[0], tx_ref[1])

    def transform(plane, carry):
        pieces = []
        for part in range(2):
            if native:
                pieces.append(
                    jnp.concatenate(
                        [
                            in_ref[owner, part, pl.ds(plane, columns, stride=depth), :]
                            for owner in range(NX // columns)
                        ],
                        axis=0,
                    )
                )
            else:
                pieces.append(in_ref[plane, part])
        real, imaginary = pieces
        stacked = jnp.concatenate(
            [
                jnp.concatenate([real, imaginary], axis=1),
                jnp.concatenate([-imaginary, real], axis=1),
            ],
            axis=0,
        )
        along_x = dot3(table_x, split(stacked))
        high, low = split(dot3(split(along_x), table_y))
        high_ref[plane] = high
        low_ref[plane] = low
        return carry

    lax.fori_loop(0, depth, transform, 0)

    for part in range(2):
        lanes = slice(part * NY, (part + 1) * NY)
        for distance in range(sets):
            record = atoms_ref[distance, part]
            rows_y = split(stencil_rows(record, CELL_Y, WY, NY))
            steep_y = split(stencil_rows(record, CELL_Y, SY, NY))
            sums_ref[...] = jnp.zeros(sums_ref.shape, jnp.float32)

            def one_plane(plane, carry):
                values = (high_ref[plane, :, lanes], low_ref[plane, :, lanes])
                weight = plane_row(record, WZ, plane, distance * depth)
                slope = plane_row(record, SZ, plane, distance * depth)
                along = dot3(values, rows_y)
                sums_ref[0] += weight * along
                sums_ref[1] += slope * along
                sums_ref[2] += weight * dot3(values, steep_y)
                return carry

            lax.fori_loop(0, planes_reached(distance, depth), one_plane, 0)
            rows_x = stencil_rows(record, CELL_X, WX, NX)
            steep_x = stencil_rows(record, CELL_X, SX, NX)
            charge = record[CHARGE : CHARGE + 1]
            level = sums_ref[0]

            def total(value):
                return jnp.sum(value, axis=0, keepdims=True)

            out_ref[distance, part] = jnp.concatenate(
                [
                    total(rows_x * level),
                    -charge * total(steep_x * level),
                    -charge * total(rows_x * sums_ref[2]),
                    -charge * total(rows_x * sums_ref[1]),
                    jnp.zeros((4, atoms), jnp.float32),
                ],
                axis=0,
            )


def influence_block(first_column, column_count):
    def frequency(counter, length):
        return jnp.where(counter >= length // 2, counter - length, counter).astype(
            jnp.float32
        ) / length

    freq_x = frequency(first_column + jnp.arange(column_count, dtype=jnp.int32), NX)[:, None, None]
    freq_z = frequency(jnp.arange(NZ, dtype=jnp.int32), NZ)[None, :, None]
    freq_y = frequency(jnp.arange(NY, dtype=jnp.int32), NY)[None, None, :]
    squared = freq_z * freq_z + freq_x * freq_x + freq_y * freq_y
    positive = squared > 0
    safe_value = jnp.where(positive, squared, jnp.float32(1.0))
    return jnp.where(
        positive,
        jnp.exp(-gauss_width * squared) / (np.pi * NX * NY * NZ * safe_value),
        jnp.float32(0.0),
    )


def body(lambdas, charge_a, charge_b, perturbed, grid_index, spline_weights, spline_slopes):
    windows, atoms = charge_a.shape
    slabs = lax.axis_size("slab")
    depth = NZ // slabs
    columns = NX // slabs
    native = depth % 8 == 0 and columns % 8 == 0
    me = lax.axis_index("slab")
    flags = perturbed.astype(jnp.float32)
    steps = flags * (charge_b - charge_a)
    charges = charge_a + flags * lambdas[:, None] * (charge_b - charge_a)

    cells = jnp.stack([grid_index[0], grid_index[1], grid_index[2] - me * depth], axis=1)
    blank = jnp.zeros((windows, 3, atoms), jnp.float32)
    record = jnp.concatenate(
        [charges[:, None], steps[:, None], cells.astype(jnp.float32), blank]
        + [jnp.moveaxis(spline_weights[d], 1, 0) for d in range(3)]
        + [jnp.moveaxis(spline_slopes[d], 1, 0) for d in range(3)],
        axis=1,
    )
    if windows % 2:
        record = jnp.pad(record, ((0, 1), (0, 0), (0, 0)))
    groups = record.shape[0] // 2
    reach = -(-REACH // depth)
    records = jnp.stack(
        [record] + [passed_along(record, "slab", distance) for distance in range(1, reach + 1)]
    )

    cos_x, sin_x = trig(NX)
    cos_y, sin_y = trig(NY)
    cos_z, sin_z = trig(NZ)
    table_x = halves(np.block([cos_x, sin_x]))
    forward_y = halves(np.block([[cos_y, -sin_y], [sin_y, cos_y]]))
    inverse_y = halves(np.block([[cos_y, sin_y], [-sin_y, cos_y]]))
    forward_z = halves(np.block([[cos_z, sin_z], [-sin_z, cos_z]]))
    inverse_z = halves(np.block([[cos_z, -sin_z], [sin_z, cos_z]]))
    influence = influence_block(me * columns, columns)

    if native:
        slab_shape = (slabs, 2, columns * depth, NY)
    else:
        slab_shape = (depth, 2, NX, NY)
    column_shape = (slabs, 2, columns * depth, NY) if native else (1, 2, columns * NZ, NY)

    cost = pl.CostEstimate(flops=8 * 10**9, bytes_accessed=4 * 10**6, transcendentals=0)

    def call(kernel, shape, scratch=()):
        return pl.pallas_call(
            kernel,
            out_shape=jax.ShapeDtypeStruct(shape, jnp.float32),
            scratch_shapes=scratch,
            cost_estimate=cost,
        )

    def to_columns(value):
        if native:
            return lax.all_to_all(value, "slab", 0, 0, tiled=True)
        value = lax.all_to_all(value, "slab", 2, 0, tiled=True)
        return jnp.transpose(value, (1, 2, 0, 3)).reshape(column_shape)

    def to_planes(value):
        if native:
            return lax.all_to_all(value, "slab", 0, 0, tiled=True)
        value = jnp.transpose(value.reshape(2, columns, NZ, NY), (2, 0, 1, 3))
        return lax.all_to_all(value, "slab", 0, 2, tiled=True)

    sampled = []
    for group in range(groups):
        mine = records[:, 2 * group : 2 * group + 2]
        planes = call(
            functools.partial(spread_kernel, depth, columns, native),
            slab_shape,
            [pltpu.VMEM((depth, NX, 2 * NY), jnp.float32)],
        )(mine, forward_y, table_x)
        back = call(functools.partial(column_kernel, columns), column_shape)(
            to_columns(planes), influence, forward_z, inverse_z
        )
        sampled.append(
            call(
                functools.partial(sample_kernel, depth, columns, native),
                (reach + 1, 2, 8, atoms),
                [
                    pltpu.VMEM((depth, NX, 2 * NY), jnp.bfloat16),
                    pltpu.VMEM((depth, NX, 2 * NY), jnp.bfloat16),
                    pltpu.VMEM((3, NX, atoms), jnp.float32),
                ],
            )(to_planes(back), mine, inverse_y, table_x)
        )
    results = jnp.concatenate(sampled, axis=1)[:, :windows]
    partial_sums = jnp.sum(
        results[:, :, :1] * records[:, :windows, CHARGE : STEP + 1], axis=(0, 3)
    )
    sums = jnp.sum(lax.all_gather(partial_sums, "slab"), axis=0)
    forces = results[0, :, 1:4]
    for distance in range(1, reach + 1):
        forces = forces + passed_along(results[distance, :, 1:4], "slab", -distance)
    total = atoms * slabs
    return (jnp.moveaxis(forces, 1, 0), 0.5 * sums[:, 0] / total, sums[:, 1] / total)


def solution(mesh):
    return jax.shard_map(
        body,
        mesh=mesh,
        in_specs=(
            P("win"),
            P("win", "slab"),
            P("win", "slab"),
            P("win", "slab"),
            P(None, "win", "slab"),
            P(None, None, "win", "slab"),
            P(None, None, "win", "slab"),
        ),
        out_specs=(P(None, "win", "slab"), P("win"), P("win")),
        check_vma=False,
    )
```

```python
import functools

import jax
import jax.numpy as jnp
import numpy as np
from jax import lax
from jax.experimental import pallas as pl
from jax.experimental.pallas import tpu as pltpu
from jax.sharding import PartitionSpec as P

NX = 128
NY = 128
NZ = 128
REACH = 3

gauss_width = 2.0

CHARGE, STEP, CELL_X, CELL_Y, CELL_Z = 0, 1, 2, 3, 4
WX, WY, WZ, SX, SY, SZ = 8, 12, 16, 20, 24, 28
BATCH = 4


def passed_along(value, axis, steps):
    count = lax.axis_size(axis)
    pairs = [(source, (source + steps) % count) for source in range(count)]
    return lax.ppermute(value, axis, pairs)


def trig(length):
    counter = np.arange(length)
    angles = (np.outer(counter, counter) % length) * (2.0 * np.pi / length)
    return np.cos(angles), np.sin(angles)


def halves(table):
    table = table.astype(np.float32)
    high = table.astype(jnp.bfloat16)
    low = (table - high.astype(np.float32)).astype(jnp.bfloat16)
    return jnp.asarray(np.stack([high, low]))


def split(value):
    high = value.astype(jnp.bfloat16)
    return high, (value - high.astype(jnp.float32)).astype(jnp.bfloat16)


def dot3(left, right, dims=((1,), (0,))):
    one = functools.partial(
        lax.dot_general, dimension_numbers=(dims, ((), ())), preferred_element_type=jnp.float32
    )
    return one(left[0], right[0]) + (one(left[0], right[1]) + one(left[1], right[0]))


def stencil_rows(record, cell_row, weight_row, length):
    first = record[cell_row : cell_row + 1].astype(jnp.int32)
    cells = lax.broadcasted_iota(jnp.int32, (length, record.shape[1]), 0)
    away = cells - first
    away = jnp.where(away < 0, away + length, away)
    result = jnp.zeros(away.shape, jnp.float32)
    for offset in range(4):
        row = weight_row + offset
        result = jnp.where(away == offset, record[row : row + 1], result)
    return result


def plane_row(record, weight_row, plane, shift):
    away = plane + shift - record[CELL_Z : CELL_Z + 1].astype(jnp.int32)
    result = jnp.zeros(away.shape, jnp.float32)
    for offset in range(4):
        row = weight_row + offset
        result = jnp.where(away == offset, record[row : row + 1], result)
    return result


def planes_reached(distance, depth):
    if distance == 0:
        return depth
    return min(depth, depth + REACH - distance * depth)


def planes_at_once(count):
    return max(size for size in range(1, BATCH + 1) if count % size == 0)


def spread_kernel(depth, columns, native, atoms_ref, ty_ref, tx_ref, out_ref, grid_ref):
    sets = atoms_ref.shape[0]

    def one_window(part, carry):
        for distance in range(sets):
            record = atoms_ref[distance, part]
            rows_x = stencil_rows(record, CELL_X, WX, NX)
            rows_y = jnp.concatenate(split(stencil_rows(record, CELL_Y, WY, NY)), axis=0)
            charge = record[CHARGE : CHARGE + 1]
            count = planes_reached(distance, depth)
            size = planes_at_once(count)

            def some_planes(step, carry):
                high, low = [], []
                for k in range(size):
                    plane = step * size + k
                    strength = plane_row(record, WZ, plane, distance * depth) * charge
                    pair = split(rows_x * strength)
                    high.append(pair[0])
                    low.append(pair[1])
                products = lax.dot_general(
                    jnp.concatenate(high + low, axis=0),
                    rows_y,
                    (((1,), (1,)), ((), ())),
                    preferred_element_type=jnp.float32,
                )
                for k in range(size):
                    top, bottom = k * NX, (size + k) * NX
                    spread = products[top : top + NX, :NY] + (
                        products[top : top + NX, NY:] + products[bottom : bottom + NX, :NY]
                    )
                    if distance == 0:
                        grid_ref[part, step * size + k] = spread
                    else:
                        grid_ref[part, step * size + k] += spread
                return carry

            lax.fori_loop(0, count // size, some_planes, 0)
        return carry

    lax.fori_loop(0, 2, one_window, 0)
    table_y = (ty_ref[0], ty_ref[1])
    table_x = (tx_ref[0], tx_ref[1])
    size = planes_at_once(depth)

    def transform(step, carry):
        packed = [
            jnp.concatenate(
                [grid_ref[0, step * size + k], grid_ref[1, step * size + k]], axis=1
            )
            for k in range(size)
        ]
        rows = dot3(split(jnp.concatenate(packed, axis=0)), table_y)
        for k in range(size):
            plane = step * size + k
            along_y = rows[k * NX : (k + 1) * NX]
            real, imaginary = along_y[:, :NY], along_y[:, NY:]
            stacked = jnp.concatenate(
                [along_y, jnp.concatenate([imaginary, -real], axis=1)], axis=0
            )
            both = dot3(table_x, split(stacked))
            for part in range(2):
                lanes = slice(part * NY, (part + 1) * NY)
                if native:
                    for owner in range(NX // columns):
                        out_ref[owner, part, pl.ds(plane, columns, stride=depth), :] = both[
                            owner * columns : (owner + 1) * columns, lanes
                        ]
                else:
                    out_ref[plane, part] = both[:, lanes]
        return carry

    lax.fori_loop(0, depth // size, transform, 0)


def column_kernel(columns, in_ref, influence_ref, forward_ref, inverse_ref, out_ref):
    sources = in_ref.shape[0]
    depth = in_ref.shape[2] // columns
    group = 2 if columns % 2 == 0 else 1
    forward = (forward_ref[0], forward_ref[1])
    inverse = (inverse_ref[0], inverse_ref[1])

    def one_group(step, carry):
        sides = []
        for k in range(group):
            start = pl.multiple_of((step * group + k) * depth, depth)
            sides.append(
                jnp.concatenate(
                    [
                        in_ref[source, part, pl.ds(start, depth), :]
                        for part in range(2)
                        for source in range(sources)
                    ],
                    axis=0,
                )
            )
        spectrum = dot3(forward, split(jnp.concatenate(sides, axis=1)))
        factor = jnp.concatenate([influence_ref[step * group + k] for k in range(group)], axis=1)
        scaled = spectrum * jnp.concatenate([factor, factor], axis=0)
        back = dot3(inverse, split(scaled))
        for k in range(group):
            start = pl.multiple_of((step * group + k) * depth, depth)
            for part in range(2):
                for source in range(sources):
                    top = part * NZ + source * depth
                    out_ref[source, part, pl.ds(start, depth), :] = back[
                        top : top + depth, k * NY : (k + 1) * NY
                    ]
        return carry

    lax.fori_loop(0, columns // group, one_group, 0)


def sample_kernel(
    depth, columns, native, in_ref, atoms_ref, ty_ref, tx_ref, out_ref, values_ref, sums_ref
):
    sets = atoms_ref.shape[0]
    atoms = atoms_ref.shape[3]
    table_y = (ty_ref[0], ty_ref[1])
    table_x = (tx_ref[0], tx_ref[1])
    size = planes_at_once(depth)

    def transform(step, carry):
        rows = []
        for k in range(size):
            plane = step * size + k
            pieces = []
            for part in range(2):
                if native:
                    pieces.append(
                        jnp.concatenate(
                            [
                                in_ref[owner, part, pl.ds(plane, columns, stride=depth), :]
                                for owner in range(NX // columns)
                            ],
                            axis=0,
                        )
                    )
                else:
                    pieces.append(in_ref[plane, part])
            real, imaginary = pieces
            stacked = jnp.concatenate(
                [
                    jnp.concatenate([real, imaginary], axis=1),
                    jnp.concatenate([-imaginary, real], axis=1),
                ],
                axis=0,
            )
            rows.append(dot3(table_x, split(stacked)))
        high, low = split(dot3(split(jnp.concatenate(rows, axis=0)), table_y))
        for k in range(size):
            span = slice(k * NX, (k + 1) * NX)
            for part in range(2):
                lanes = slice(part * NY, (part + 1) * NY)
                values_ref[part, step * size + k] = jnp.concatenate(
                    [high[span, lanes], low[span, lanes]], axis=1
                )
        return carry

    lax.fori_loop(0, depth // size, transform, 0)

    def one_window(part, carry):
        for distance in range(sets):
            record = atoms_ref[distance, part]
            high_y, low_y = split(
                jnp.concatenate(
                    [
                        stencil_rows(record, CELL_Y, WY, NY),
                        stencil_rows(record, CELL_Y, SY, NY),
                    ],
                    axis=1,
                )
            )
            both_y = jnp.concatenate([high_y, high_y], axis=0)
            sums_ref[...] = jnp.zeros(sums_ref.shape, jnp.float32)
            count = planes_reached(distance, depth)
            size = planes_at_once(count)

            def some_planes(step, carry):
                first = step * size
                values = jnp.concatenate(
                    [values_ref[part, first + k] for k in range(size)], axis=0
                )
                along = jnp.dot(values, both_y, preferred_element_type=jnp.float32) + jnp.dot(
                    values[:, :NY], low_y, preferred_element_type=jnp.float32
                )
                level, rise, across = sums_ref[0], sums_ref[1], sums_ref[2]
                for k in range(size):
                    weight = plane_row(record, WZ, first + k, distance * depth)
                    slope = plane_row(record, SZ, first + k, distance * depth)
                    plain = along[k * NX : (k + 1) * NX, :atoms]
                    level += weight * plain
                    rise += slope * plain
                    across += weight * along[k * NX : (k + 1) * NX, atoms:]
                sums_ref[0] = level
                sums_ref[1] = rise
                sums_ref[2] = across
                return carry

            lax.fori_loop(0, count // size, some_planes, 0)
            rows_x = stencil_rows(record, CELL_X, WX, NX)
            steep_x = stencil_rows(record, CELL_X, SX, NX)
            charge = record[CHARGE : CHARGE + 1]
            level = sums_ref[0]

            def total(value):
                return jnp.sum(value, axis=0, keepdims=True)

            out_ref[distance, part] = jnp.concatenate(
                [
                    total(rows_x * level),
                    -charge * total(steep_x * level),
                    -charge * total(rows_x * sums_ref[2]),
                    -charge * total(rows_x * sums_ref[1]),
                    jnp.zeros((4, atoms), jnp.float32),
                ],
                axis=0,
            )
        return carry

    lax.fori_loop(0, 2, one_window, 0)


def influence_block(first_column, column_count):
    def frequency(counter, length):
        return jnp.where(counter >= length // 2, counter - length, counter).astype(
            jnp.float32
        ) / length

    freq_x = frequency(first_column + jnp.arange(column_count, dtype=jnp.int32), NX)[:, None, None]
    freq_z = frequency(jnp.arange(NZ, dtype=jnp.int32), NZ)[None, :, None]
    freq_y = frequency(jnp.arange(NY, dtype=jnp.int32), NY)[None, None, :]
    squared = freq_z * freq_z + freq_x * freq_x + freq_y * freq_y
    positive = squared > 0
    safe_value = jnp.where(positive, squared, jnp.float32(1.0))
    return jnp.where(
        positive,
        jnp.exp(-gauss_width * squared) / (np.pi * NX * NY * NZ * safe_value),
        jnp.float32(0.0),
    )


def body(lambdas, charge_a, charge_b, perturbed, grid_index, spline_weights, spline_slopes):
    windows, atoms = charge_a.shape
    slabs = lax.axis_size("slab")
    depth = NZ // slabs
    columns = NX // slabs
    native = depth % 8 == 0 and columns % 8 == 0
    me = lax.axis_index("slab")
    flags = perturbed.astype(jnp.float32)
    steps = flags * (charge_b - charge_a)
    charges = charge_a + flags * lambdas[:, None] * (charge_b - charge_a)

    cells = jnp.stack([grid_index[0], grid_index[1], grid_index[2] - me * depth], axis=1)
    blank = jnp.zeros((windows, 3, atoms), jnp.float32)
    record = jnp.concatenate(
        [charges[:, None], steps[:, None], cells.astype(jnp.float32), blank]
        + [jnp.moveaxis(spline_weights[d], 1, 0) for d in range(3)]
        + [jnp.moveaxis(spline_slopes[d], 1, 0) for d in range(3)],
        axis=1,
    )
    if windows % 2:
        record = jnp.pad(record, ((0, 1), (0, 0), (0, 0)))
    groups = record.shape[0] // 2
    reach = -(-REACH // depth)
    records = jnp.stack(
        [record] + [passed_along(record, "slab", distance) for distance in range(1, reach + 1)]
    )

    cos_x, sin_x = trig(NX)
    cos_y, sin_y = trig(NY)
    cos_z, sin_z = trig(NZ)
    table_x = halves(np.block([cos_x, sin_x]))
    forward_y = halves(np.block([[cos_y, -sin_y], [sin_y, cos_y]]))
    inverse_y = halves(np.block([[cos_y, sin_y], [-sin_y, cos_y]]))
    forward_z = halves(np.block([[cos_z, sin_z], [-sin_z, cos_z]]))
    inverse_z = halves(np.block([[cos_z, -sin_z], [sin_z, cos_z]]))
    influence = influence_block(me * columns, columns)

    if native:
        slab_shape = (slabs, 2, columns * depth, NY)
    else:
        slab_shape = (depth, 2, NX, NY)
    column_shape = (slabs, 2, columns * depth, NY) if native else (1, 2, columns * NZ, NY)

    cost = pl.CostEstimate(flops=8 * 10**9, bytes_accessed=4 * 10**6, transcendentals=0)

    def call(kernel, shape, scratch=()):
        return pl.pallas_call(
            kernel,
            out_shape=jax.ShapeDtypeStruct(shape, jnp.float32),
            scratch_shapes=scratch,
            cost_estimate=cost,
        )

    def to_columns(value):
        if native:
            return lax.all_to_all(value, "slab", 0, 0, tiled=True)
        value = lax.all_to_all(value, "slab", 2, 0, tiled=True)
        return jnp.transpose(value, (1, 2, 0, 3)).reshape(column_shape)

    def to_planes(value):
        if native:
            return lax.all_to_all(value, "slab", 0, 0, tiled=True)
        value = jnp.transpose(value.reshape(2, columns, NZ, NY), (2, 0, 1, 3))
        return lax.all_to_all(value, "slab", 0, 2, tiled=True)

    sampled = []
    for group in range(groups):
        mine = records[:, 2 * group : 2 * group + 2]
        planes = call(
            functools.partial(spread_kernel, depth, columns, native),
            slab_shape,
            [pltpu.VMEM((2, depth, NX, NY), jnp.float32)],
        )(mine, forward_y, table_x)
        back = call(functools.partial(column_kernel, columns), column_shape)(
            to_columns(planes), influence, forward_z, inverse_z
        )
        sampled.append(
            call(
                functools.partial(sample_kernel, depth, columns, native),
                (reach + 1, 2, 8, atoms),
                [
                    pltpu.VMEM((2, depth, NX, 2 * NY), jnp.bfloat16),
                    pltpu.VMEM((3, NX, atoms), jnp.float32),
                ],
            )(to_planes(back), mine, inverse_y, table_x)
        )
    results = jnp.concatenate(sampled, axis=1)[:, :windows]
    partial_sums = jnp.sum(
        results[:, :, :1] * records[:, :windows, CHARGE : STEP + 1], axis=(0, 3)
    )
    copies = jnp.broadcast_to(partial_sums[None], (slabs,) + partial_sums.shape)
    sums = jnp.sum(lax.all_to_all(copies, "slab", 0, 0, tiled=True), axis=0)
    forces = results[0, :, 1:4]
    for distance in range(1, reach + 1):
        forces = forces + passed_along(results[distance, :, 1:4], "slab", -distance)
    total = atoms * slabs
    return (jnp.moveaxis(forces, 1, 0), 0.5 * sums[:, 0] / total, sums[:, 1] / total)


def solution(mesh):
    return jax.shard_map(
        body,
        mesh=mesh,
        in_specs=(
            P("win"),
            P("win", "slab"),
            P("win", "slab"),
            P("win", "slab"),
            P(None, "win", "slab"),
            P(None, None, "win", "slab"),
            P(None, None, "win", "slab"),
        ),
        out_specs=(P(None, "win", "slab"), P("win"), P("win")),
        check_vma=False,
    )
```
